32 devices in a mesh: z: 4 (over z), y: 2 (over y), xc: 4 (over x, core).
Axes of the slice: x: 2, y: 2, z: 4, core: 2. Of those that a mesh axis runs over, the one named last changes fastest.
Arguments:
- tokens_x: bfloat16 [262144, 512], P(('z', 'y', 'xc'))
- grad_y: bfloat16 [262144, 512], P(('z', 'y', 'xc'))
- w_one: bfloat16 [512, 2048], replicated
- w_two: bfloat16 [2048, 512], replicated
- w_three: bfloat16 [512, 2048], replicated
- w_four: bfloat16 [2048, 512], replicated
Outputs:
- output 1: float32 [512, 2048], replicated
- output 2: float32 [2048, 512], replicated
- output 3: float32 [512, 2048], replicated
- output 4: float32 [2048, 512], replicated
All inputs are finite; a program needn't handle non-finite values.
Results may differ from the reference program's by a relative error of at most 0.0033.
Values are sent between devices in bfloat16 or wider.
A program may use at most 1 GiB of HBM per device.

```python
import math
import jax
import jax.numpy as jnp
from jax import lax

D = 512
FF = 2048
TOKENS_DEV = 8192
DEVICES = 32

TOKENS = DEVICES * TOKENS_DEV
GELU_SCALE = math.sqrt(2.0 / math.pi)
GELU_CUBIC = 0.044715


def gelu_value(pre_act):
    return 0.5 * pre_act * (1.0 + jnp.tanh(GELU_SCALE * (pre_act + GELU_CUBIC * pre_act * pre_act * pre_act)))


def gelu_grad(pre_act):
    tanh_val = jnp.tanh(GELU_SCALE * (pre_act + GELU_CUBIC * pre_act * pre_act * pre_act))
    return 0.5 * (1.0 + tanh_val) + 0.5 * pre_act * (1.0 - tanh_val * tanh_val) * GELU_SCALE * (1.0 + 3.0 * GELU_CUBIC * pre_act * pre_act)


def setup_inputs(seed: int = 0) -> dict:
    root_key = jax.random.key(seed)
    key_list = jax.random.split(root_key, 8)
    scale_x = jax.random.uniform(key_list[0], (DEVICES, 1, 1), jnp.float32, 0.7, 1.3)
    scale_g = jax.random.uniform(key_list[1], (DEVICES, 1, 1), jnp.float32, 0.7, 1.3)
    x_rows = jax.random.normal(key_list[2], (DEVICES, TOKENS_DEV, D), jnp.float32) * scale_x
    g_rows = jax.random.normal(key_list[3], (DEVICES, TOKENS_DEV, D), jnp.float32) * scale_g
    w_one = jax.random.normal(key_list[4], (D, FF), jnp.float32) * D ** -0.5
    w_two = jax.random.normal(key_list[5], (FF, D), jnp.float32) * FF ** -0.5
    w_three = jax.random.normal(key_list[6], (D, FF), jnp.float32) * D ** -0.5
    w_four = jax.random.normal(key_list[7], (FF, D), jnp.float32) * FF ** -0.5
    return {
        "tokens_x": x_rows.reshape(TOKENS, D).astype(jnp.bfloat16),
        "grad_y": g_rows.reshape(TOKENS, D).astype(jnp.bfloat16),
        "w_one": w_one.astype(jnp.bfloat16),
        "w_two": w_two.astype(jnp.bfloat16),
        "w_three": w_three.astype(jnp.bfloat16),
        "w_four": w_four.astype(jnp.bfloat16),
    }


def local_grads(x_loc, g_loc, w_one, w_two, w_three, w_four):
    a_one = jnp.dot(x_loc, w_one, preferred_element_type=jnp.float32).astype(jnp.bfloat16)
    h_one = gelu_value(a_one.astype(jnp.float32)).astype(jnp.bfloat16)
    h_two = (jnp.dot(h_one, w_two, preferred_element_type=jnp.float32) + x_loc.astype(jnp.float32)).astype(jnp.bfloat16)
    a_three = jnp.dot(h_two, w_three, preferred_element_type=jnp.float32).astype(jnp.bfloat16)
    h_three = gelu_value(a_three.astype(jnp.float32)).astype(jnp.bfloat16)
    d_w4 = jnp.dot(h_three.T, g_loc, preferred_element_type=jnp.float32)
    d_a3 = (jnp.dot(g_loc, w_four.T, preferred_element_type=jnp.float32) * gelu_grad(a_three.astype(jnp.float32))).astype(jnp.bfloat16)
    d_w3 = jnp.dot(h_two.T, d_a3, preferred_element_type=jnp.float32)
    d_h2 = (jnp.dot(d_a3, w_three.T, preferred_element_type=jnp.float32) + g_loc.astype(jnp.float32)).astype(jnp.bfloat16)
    d_w2 = jnp.dot(h_one.T, d_h2, preferred_element_type=jnp.float32)
    d_a1 = (jnp.dot(d_h2, w_two.T, preferred_element_type=jnp.float32) * gelu_grad(a_one.astype(jnp.float32))).astype(jnp.bfloat16)
    d_w1 = jnp.dot(x_loc.T, d_a1, preferred_element_type=jnp.float32)
    return d_w1, d_w2, d_w3, d_w4


def reference(tokens_x, grad_y, w_one, w_two, w_three, w_four):
    x_shards = tokens_x.reshape(DEVICES, TOKENS_DEV, D)
    g_shards = grad_y.reshape(DEVICES, TOKENS_DEV, D)

    def accumulate(running, pair):
        x_loc, g_loc = pair
        grads = local_grads(x_loc, g_loc, w_one, w_two, w_three, w_four)
        return tuple(acc + new for acc, new in zip(running, grads)), None

    start_sums = (
        jnp.zeros((D, FF), jnp.float32),
        jnp.zeros((FF, D), jnp.float32),
        jnp.zeros((D, FF), jnp.float32),
        jnp.zeros((FF, D), jnp.float32),
    )
    totals, _ = lax.scan(accumulate, start_sums, (x_shards, g_shards))
    return (totals[0] / DEVICES, totals[1] / DEVICES, totals[2] / DEVICES, totals[3] / DEVICES)
```

```python
import functools
import math
import jax
import jax.numpy as jnp
from jax import lax
from jax.experimental import pallas as pl
from jax.experimental.pallas import tpu as pltpu
from jax.sharding import PartitionSpec as P

C0 = math.sqrt(2.0 / math.pi)
K0 = 0.044715
F32 = jnp.float32
BF16 = jnp.bfloat16
MESH = pl.DeviceIdType.MESH
VMEM_LIMIT = 67_000_000

NCH = 4
NRB = 8
UNITS = 2 * NCH
SLOTS = 4
SUBS = 2

OFF = dict(d=0, s1=2, s2=6, z=9, zg=14, s2g=19, s1g=22, dg=26, end=29)


def nn(a, b):
    return jnp.dot(a, b, preferred_element_type=F32)


def nt(a, b):
    return lax.dot_general(a, b, (((1,), (1,)), ((), ())), preferred_element_type=F32)


def tn(a, b):
    return lax.dot_general(a, b, (((0,), (0,)), ((), ())), preferred_element_type=F32)


def gelu_only(a):
    kq = (K0 * a) * a
    t = jnp.tanh((C0 * a) * (1.0 + kq))
    return a * (0.5 * t + 0.5)


def gelu_both(a):
    kq = (K0 * a) * a
    t = jnp.tanh((C0 * a) * (1.0 + kq))
    s = 0.5 * t + 0.5
    h = a * s
    grad = s + (h * (C0 - C0 * t)) * (1.0 + 3.0 * kq)
    return h, grad


def fwd_kernel(x_ref, w1_ref, w2_ref, a1_ref, h2_ref):
    ffc = w1_ref.shape[1] // NCH
    x = x_ref[...]
    acc = x.astype(F32)
    for c in range(NCH):
        cols = slice(c * ffc, (c + 1) * ffc)
        a1 = nn(x, w1_ref[:, cols]).astype(BF16)
        a1_ref[:, cols] = a1
        h1 = gelu_only(a1.astype(F32)).astype(BF16)
        acc += nn(h1, w2_ref[cols, :])
    h2_ref[...] = acc.astype(BF16)


def grad_kernel(
    x_hbm, g_hbm, h2_hbm, a1_hbm, w2_hbm, w3_hbm, w4_hbm, o_hbm,
    h2, gx, dh, w2, w3, w4, a1b, pb, q, r1, r2, rz,
    wsem, hsem, gsem, xsem, asem, lsem, ssem, rsem, csem,
):
    d = h2.shape[1]
    rows = h2.shape[0] // NRB
    ffc = w3.shape[1] // NCH
    half, col, s1n, s2n, zn = d // 2, d // 4, d // 8, d // 16, d // 64

    xc, y, z = lax.axis_index("xc"), lax.axis_index("y"), lax.axis_index("z")
    x, core = lax.div(xc, 2), lax.rem(xc, 2)
    to_core = {"xc": xc + 1 - 2 * core}
    to_x = {"xc": core + 2 * (1 - x)}
    to_y = {"y": 1 - y}
    to_z = [{"z": lax.rem(z + j, 4)} for j in (1, 2, 3)]
    peers = [to_core, to_x, to_y] + to_z

    def al(v, m):
        return pl.multiple_of(v, m)

    def block(i):
        return pl.ds(al(i * rows, rows), rows)

    w_copies = [
        pltpu.make_async_copy(src, dst, wsem.at[i])
        for i, (src, dst) in enumerate(((w3_hbm, w3), (w4_hbm, w4), (w2_hbm, w2)))
    ]

    def h_copy(i):
        return pltpu.make_async_copy(h2_hbm.at[block(i)], h2.at[block(i)], hsem.at[i])

    def g_copy(i):
        return pltpu.make_async_copy(g_hbm.at[block(i)], gx.at[block(i)], gsem.at[i])

    def x_copy(i):
        return pltpu.make_async_copy(x_hbm.at[block(i)], gx.at[block(i)], xsem.at[i])

    def a_copy(i):
        c, r = lax.div(i, NRB), lax.rem(i, NRB)
        slot = lax.rem(i, 2)
        return pltpu.make_async_copy(
            a1_hbm.at[block(r), pl.ds(al(c * ffc, ffc), ffc)], a1b.at[slot], asem.at[slot]
        )

    w_copies[0].start()
    h_copy(0).start()
    w_copies[1].start()
    g_copy(0).start()
    for i in range(1, NRB):
        h_copy(i).start()
        g_copy(i).start()
    w_copies[2].start()
    a_copy(jnp.int32(0)).start()

    barrier = pltpu.get_barrier_semaphore()
    for peer in peers:
        pl.semaphore_signal(barrier, inc=1, device_id=peer, device_id_type=MESH)
    pl.semaphore_wait(barrier, len(peers))

    xa, yb = x * s1n, col + y * s1n
    xya, yxb = xa + y * s2n, yb + x * s2n

    def remote(src, dst, k, i, peer):
        return pltpu.make_async_remote_copy(
            src_ref=src, dst_ref=dst, send_sem=ssem.at[k, i], recv_sem=rsem.at[k, i],
            device_id=peer, device_id_type=MESH,
        )

    def c_d(k):
        return [remote(
            pb.at[lax.rem(k, 2), :, pl.ds(al((1 - core) * half, half), half), :],
            q.at[lax.rem(k, SLOTS)], k, 0, to_core)]

    def q_at(k, start, size):
        return q.at[lax.rem(k, SLOTS), :, pl.ds(al(start, zn), size), :]

    def o_at(k, start, size):
        return o_hbm.at[k, :, pl.ds(al(core * half + start, zn), size), :]

    def c_s1(k):
        sl = lax.rem(k, SLOTS)
        return [
            remote(q_at(k, (1 - x) * s1n, s1n), r1.at[sl, 0], k, 1, to_x),
            remote(q_at(k, col + (1 - y) * s1n, s1n), r1.at[sl, 1], k, 2, to_y),
        ]

    def c_s2(k):
        sl = lax.rem(k, SLOTS)
        return [
            remote(q_at(k, xa + (1 - y) * s2n, s2n), r2.at[sl, 0], k, 3, to_y),
            remote(q_at(k, yb + (1 - x) * s2n, s2n), r2.at[sl, 1], k, 4, to_x),
        ]

    def c_z(k):
        sl = lax.rem(k, SLOTS)
        out = []
        for j in range(3):
            zz = lax.rem(z + j + 1, 4) * zn
            out.append(remote(q_at(k, xya + zz, zn), rz.at[sl, j, 0], k, 5 + 2 * j, to_z[j]))
            out.append(remote(q_at(k, yxb + zz, zn), rz.at[sl, j, 1], k, 6 + 2 * j, to_z[j]))
        return out

    def c_zg(k):
        out = []
        for j in range(3):
            for n, base in enumerate((xya, yxb)):
                at = base + z * zn
                out.append(remote(q_at(k, at, zn), o_at(k, at, zn), k, 11 + 2 * j + n, to_z[j]))
        return out

    def c_local(k):
        return [
            pltpu.make_async_copy(q_at(k, base + z * zn, zn), o_at(k, base + z * zn, zn), lsem.at[k, n])
            for n, base in enumerate((xya, yxb))
        ]

    def c_s2g(k):
        return [
            remote(o_at(k, xya, s2n), o_at(k, xya, s2n), k, 17, to_y),
            remote(o_at(k, yxb, s2n), o_at(k, yxb, s2n), k, 18, to_x),
        ]

    def c_s1g(k):
        return [
            remote(o_at(k, xa, s1n), o_at(k, xa, s1n), k, 19, to_x),
            remote(o_at(k, yb, s1n), o_at(k, yb, s1n), k, 20, to_y),
        ]

    def c_dg(k):
        return [remote(o_at(k, 0, half), o_at(k, 0, half), k, 21, to_core)]

    def start(copies):
        for copy in copies:
            copy.start()

    def wait(copies):
        for copy in copies:
            copy.wait()

    def q_add(k, at, size, value):
        sl = lax.rem(k, SLOTS)
        ds = pl.ds(al(at, zn), size)
        q[sl, :, ds, :] = q[sl, :, ds, :] + value

    def stage(g, name, action):
        t = g - OFF[name] - NRB
        k = lax.div(t, NRB)

        @pl.when((t >= 0) & (lax.rem(t, NRB) == 0) & (k < UNITS))
        def _():
            action(k)

    def do_d(k):
        @pl.when(k >= SLOTS)
        def _():
            pl.semaphore_wait(csem.at[lax.rem(k, SLOTS)], len(peers))
        start(c_d(k))

    def do_s1(k):
        wait(c_d(k))
        sl = lax.rem(k, SLOTS)
        q[sl] = q[sl] + pb[lax.rem(k, 2), :, pl.ds(al(core * half, half), half), :]
        start(c_s1(k))

    def do_s2(k):
        wait(c_s1(k))
        sl = lax.rem(k, SLOTS)
        q_add(k, xa, s1n, r1[sl, 0])
        q_add(k, yb, s1n, r1[sl, 1])
        start(c_s2(k))

    def do_z(k):
        wait(c_s2(k))
        sl = lax.rem(k, SLOTS)
        q_add(k, xya, s2n, r2[sl, 0])
        q_add(k, yxb, s2n, r2[sl, 1])
        start(c_z(k))

    def do_zg(k):
        wait(c_z(k))
        sl = lax.rem(k, SLOTS)
        for n, base in enumerate((xya, yxb)):
            ds = pl.ds(al(base + z * zn, zn), zn)
            total = (q[sl, :, ds, :] + rz[sl, 0, n]) + (rz[sl, 1, n] + rz[sl, 2, n])
            q[sl, :, ds, :] = total * (1.0 / 32.0)
        start(c_zg(k))
        start(c_local(k))

    def do_s2g(k):
        wait(c_zg(k))
        wait(c_local(k))

        @pl.when(k < UNITS - SLOTS)
        def _():
            for peer in peers:
                pl.semaphore_signal(csem.at[lax.rem(k, SLOTS)], inc=1, device_id=peer, device_id_type=MESH)
        start(c_s2g(k))

    def do_s1g(k):
        wait(c_s2g(k))
        start(c_s1g(k))

    def do_dg(k):
        wait(c_s1g(k))
        start(c_dg(k))

    def do_end(k):
        wait(c_dg(k))

    def comm(g):
        stage(g, "d", do_d)
        stage(g, "end", do_end)
        stage(g, "dg", do_dg)
        stage(g, "s1g", do_s1g)
        stage(g, "s2g", do_s2g)
        stage(g, "zg", do_zg)
        stage(g, "z", do_z)
        stage(g, "s2", do_s2)
        stage(g, "s1", do_s1)

    sub = rows // SUBS

    def first_step(g, carry):
        c, r = lax.div(g, NRB), lax.rem(g, NRB)
        par = lax.rem(c, 2)
        comm(g)

        @pl.when(g == 0)
        def _():
            w_copies[0].wait()
            w_copies[1].wait()

        @pl.when(c == 0)
        def _():
            h_copy(r).wait()
            g_copy(r).wait()

        @pl.when(r == 0)
        def _():
            pb[par] = jnp.zeros_like(pb[par])

        cols = pl.ds(al(c * ffc, ffc), ffc)
        wc3 = w3[:, cols]
        wc4 = w4[cols, :]
        for i in range(SUBS):
            ds = pl.ds(al(r * rows + i * sub, sub), sub)
            h2r, gr = h2[ds, :], gx[ds, :]
            a3 = nn(h2r, wc3).astype(BF16).astype(F32)
            u = nt(gr, wc4)
            h3, da = gelu_both(a3)
            h3 = h3.astype(BF16)
            da = (u * da).astype(BF16)
            pb[par, 0] += tn(h3, gr)
            pb[par, 1] += tn(h2r, da)
            prev = jnp.where(c == 0, gr.astype(F32), dh[ds, :])
            dh[ds, :] = prev + nt(da, wc3)

        @pl.when(c == NCH - 1)
        def _():
            h2[block(r), :] = dh[block(r), :].astype(BF16)
            x_copy(r).start()
        return carry

    def second_step(g, carry):
        i0 = g - NCH * NRB
        c, r = lax.div(i0, NRB), lax.rem(i0, NRB)
        par = lax.rem(c, 2)
        slot = lax.rem(i0, 2)

        @pl.when(i0 + 1 < NCH * NRB)
        def _():
            a_copy(i0 + 1).start()
        comm(g)

        @pl.when(c == 0)
        def _():
            x_copy(r).wait()

        @pl.when(r == 0)
        def _():
            pb[par] = jnp.zeros_like(pb[par])
        a_copy(i0).wait()

        wc2 = w2[pl.ds(al(c * ffc, ffc), ffc), :]
        for i in range(SUBS):
            ds = pl.ds(al(r * rows + i * sub, sub), sub)
            dr, xr = h2[ds, :], gx[ds, :]
            a1 = a1b[slot, i * sub : (i + 1) * sub, :].astype(F32)
            v = nt(dr, wc2)
            h1, da = gelu_both(a1)
            h1 = h1.astype(BF16)
            da = (v * da).astype(BF16)
            pb[par, 0] += tn(h1, dr)
            pb[par, 1] += tn(xr, da)
        return carry

    steps = NCH * NRB
    lax.fori_loop(0, steps, first_step, 0)
    w_copies[2].wait()
    lax.fori_loop(steps, 2 * steps, second_step, 0)

    def drain(g, carry):
        comm(g)
        return carry

    lax.fori_loop(2 * steps, 2 * steps + OFF["end"] + 1, drain, 0)


def solution(mesh):
    batch_spec = P(("z", "y", "xc"), None)
    whole_spec = P(None, None)
    any_spec = pl.BlockSpec(memory_space=pl.ANY)

    def device_step(x_loc, g_loc, w_one, w_two, w_three, w_four):
        n, d = x_loc.shape
        ff = w_one.shape[1]
        rows, ffc = n // NRB, ff // NCH
        mm = 2 * n * d * ff
        a1, h2 = pl.pallas_call(
            fwd_kernel,
            grid=(NRB,),
            in_specs=[
                pl.BlockSpec((rows, d), lambda i: (i, 0)),
                pl.BlockSpec((d, ff), lambda i: (0, 0)),
                pl.BlockSpec((ff, d), lambda i: (0, 0)),
            ],
            out_specs=[
                pl.BlockSpec((rows, ff), lambda i: (i, 0)),
                pl.BlockSpec((rows, d), lambda i: (i, 0)),
            ],
            out_shape=[jax.ShapeDtypeStruct((n, ff), BF16), jax.ShapeDtypeStruct((n, d), BF16)],
            compiler_params=pltpu.CompilerParams(vmem_limit_bytes=VMEM_LIMIT),
            cost_estimate=pl.CostEstimate(flops=2 * mm, bytes_accessed=2 * n * (ff + 2 * d), transcendentals=n * ff),
            name="fwd",
        )(x_loc, w_one, w_two)

        out = pl.pallas_call(
            grad_kernel,
            in_specs=[any_spec] * 7,
            out_specs=any_spec,
            out_shape=jax.ShapeDtypeStruct((UNITS, 2, d, ffc), F32),
            scratch_shapes=[
                pltpu.VMEM((n, d), BF16),
                pltpu.VMEM((n, d), BF16),
                pltpu.VMEM((n, d), F32),
                pltpu.VMEM((ff, d), BF16),
                pltpu.VMEM((d, ff), BF16),
                pltpu.VMEM((ff, d), BF16),
                pltpu.VMEM((2, rows, ffc), BF16),
                pltpu.VMEM((2, 2, d, ffc), F32),
                pltpu.VMEM((SLOTS, 2, d // 2, ffc), F32),
                pltpu.VMEM((SLOTS, 2, 2, d // 8, ffc), F32),
                pltpu.VMEM((SLOTS, 2, 2, d // 16, ffc), F32),
                pltpu.VMEM((SLOTS, 3, 2, 2, d // 64, ffc), F32),
                pltpu.SemaphoreType.DMA((3,)),
                pltpu.SemaphoreType.DMA((NRB,)),
                pltpu.SemaphoreType.DMA((NRB,)),
                pltpu.SemaphoreType.DMA((NRB,)),
                pltpu.SemaphoreType.DMA((2,)),
                pltpu.SemaphoreType.DMA((UNITS, 2)),
                pltpu.SemaphoreType.DMA((UNITS, 22)),
                pltpu.SemaphoreType.DMA((UNITS, 22)),
                pltpu.SemaphoreType.REGULAR((SLOTS,)),
            ],
            compiler_params=pltpu.CompilerParams(
                collective_id=0, has_side_effects=True, vmem_limit_bytes=VMEM_LIMIT
            ),
            cost_estimate=pl.CostEstimate(flops=8 * mm, bytes_accessed=2 * n * (ff + 3 * d), transcendentals=2 * n * ff),
            name="grads",
        )(x_loc, g_loc, h2, a1, w_two, w_three, w_four)

        def stack_rows(v):
            return v.reshape(ff, d)

        def stack_cols(v):
            return v.transpose(1, 0, 2).reshape(d, ff)

        return (
            stack_cols(out[NCH:, 1]),
            stack_rows(out[NCH:, 0]),
            stack_cols(out[:NCH, 1]),
            stack_rows(out[:NCH, 0]),
        )

    return jax.shard_map(
        device_step,
        mesh=mesh,
        in_specs=(batch_spec, batch_spec, whole_spec, whole_spec, whole_spec, whole_spec),
        out_specs=(whole_spec, whole_spec, whole_spec, whole_spec),
        check_vma=False,
    )
```

```python
import functools
import math
import jax
import jax.numpy as jnp
from jax import lax
from jax.experimental import pallas as pl
from jax.experimental.pallas import tpu as pltpu
from jax.sharding import PartitionSpec as P

C0 = math.sqrt(2.0 / math.pi)
K0 = 0.044715
F32 = jnp.float32
BF16 = jnp.bfloat16
MESH = pl.DeviceIdType.MESH
VMEM_LIMIT = 67_000_000

NCH = 4
NRB = 8
UNITS = 2 * NCH
SLOTS = 4
SUBS = 4
EROWS = 16

OFF = dict(d=0, s1=2, s2=6, z=9, zg=14, s2g=19, s1g=22, dg=26, end=29)


def nn(a, b):
    return jnp.dot(a, b, preferred_element_type=F32)


def nt(a, b):
    return lax.dot_general(a, b, (((1,), (1,)), ((), ())), preferred_element_type=F32)


def tn(a, b):
    return lax.dot_general(a, b, (((0,), (0,)), ((), ())), preferred_element_type=F32)


def gelu_only(a):
    kq = (K0 * a) * a
    t = jnp.tanh((C0 * a) * (1.0 + kq))
    return a * (0.5 * t + 0.5)


def gelu_both(a):
    kq = (K0 * a) * a
    t = jnp.tanh((C0 * a) * (1.0 + kq))
    s = 0.5 * t + 0.5
    h = a * s
    grad = s + (h * (C0 - C0 * t)) * (1.0 + 3.0 * kq)
    return h, grad


def woven(first, second):
    order = [((i + 0.5) / len(first), 0, f) for i, f in enumerate(first)]
    order += [((i + 0.5) / len(second), 1, f) for i, f in enumerate(second)]
    for _, _, f in sorted(order, key=lambda e: e[:2]):
        f()


def pipelined(count, front, middle, back, back_first=True):
    for f in front(0):
        f()
    for j in range(count):
        around = [front(j + 1) if j + 1 < count else [], back(j - 1) if j else []]
        around = around[1] + around[0] if back_first else around[0] + around[1]
        woven(around, middle(j))
    for f in back(count - 1):
        f()


def fwd_kernel(x_ref, w1_ref, w2_ref, a1_ref, h2_ref, hb, acc):
    rows, d = x_ref.shape
    ffc = w1_ref.shape[1] // NCH
    half = rows // 2
    er = min(EROWS, half)

    def place(j):
        c, n = j // 2, j % 2
        return slice(c * ffc, (c + 1) * ffc), slice(n * half, (n + 1) * half), c

    def front(j):
        cols, at, c = place(j)

        def up():
            a1_ref[at, cols] = nn(x_ref[at, :], w1_ref[:, cols]).astype(BF16)

        return [up]

    def middle(j):
        cols, at, c = place(j)

        def piece(i):
            ds = slice(at.start + i, at.start + i + er)
            hb[ds, cols] = gelu_only(a1_ref[ds, cols].astype(F32)).astype(BF16)

        return [functools.partial(piece, i) for i in range(0, half, er)]

    def back(j):
        cols, at, c = place(j)

        def down():
            prev = x_ref[at, :].astype(F32) if c == 0 else acc[at, :]
            total = prev + nn(hb[at, cols], w2_ref[cols, :])
            if c == NCH - 1:
                h2_ref[at, :] = total.astype(BF16)
            else:
                acc[at, :] = total

        return [down]

    pipelined(2 * NCH, front, middle, back, back_first=False)


def grad_kernel(
    x_hbm, g_hbm, h2_hbm, a1_hbm, w2_hbm, w3_hbm, w4_hbm, o_hbm,
    h2, gx, dh, w2, w3, w4, a1b, ab, ub, hb, db, pb, q, r1, r2, rz,
    wsem, hsem, gsem, xsem, asem, lsem, ssem, rsem, csem,
):
    d = h2.shape[1]
    rows = h2.shape[0] // NRB
    ffc = w3.shape[1] // NCH
    half, col, s1n, s2n, zn = d // 2, d // 4, d // 8, d // 16, d // 64

    xc, y, z = lax.axis_index("xc"), lax.axis_index("y"), lax.axis_index("z")
    x, core = lax.div(xc, 2), lax.rem(xc, 2)
    to_core = {"xc": xc + 1 - 2 * core}
    to_x = {"xc": core + 2 * (1 - x)}
    to_y = {"y": 1 - y}
    to_z = [{"z": lax.rem(z + j, 4)} for j in (1, 2, 3)]
    peers = [to_core, to_x, to_y] + to_z

    def al(v, m):
        return pl.multiple_of(v, m)

    def block(i):
        return pl.ds(al(i * rows, rows), rows)

    w_copies = [
        pltpu.make_async_copy(src, dst, wsem.at[i])
        for i, (src, dst) in enumerate(((w3_hbm, w3), (w4_hbm, w4), (w2_hbm, w2)))
    ]

    def h_copy(i):
        return pltpu.make_async_copy(h2_hbm.at[block(i)], h2.at[block(i)], hsem.at[i])

    def g_copy(i):
        return pltpu.make_async_copy(g_hbm.at[block(i)], gx.at[block(i)], gsem.at[i])

    def x_copy(i):
        return pltpu.make_async_copy(x_hbm.at[block(i)], gx.at[block(i)], xsem.at[i])

    def a_copy(i):
        c, r = lax.div(i, NRB), lax.rem(i, NRB)
        slot = lax.rem(i, 2)
        return pltpu.make_async_copy(
            a1_hbm.at[block(r), pl.ds(al(c * ffc, ffc), ffc)], a1b.at[slot], asem.at[slot]
        )

    w_copies[0].start()
    h_copy(0).start()
    w_copies[1].start()
    g_copy(0).start()
    for i in range(1, NRB):
        h_copy(i).start()
        g_copy(i).start()
    w_copies[2].start()
    a_copy(jnp.int32(0)).start()

    barrier = pltpu.get_barrier_semaphore()
    for peer in peers:
        pl.semaphore_signal(barrier, inc=1, device_id=peer, device_id_type=MESH)
    pl.semaphore_wait(barrier, len(peers))

    xa, yb = x * s1n, col + y * s1n
    xya, yxb = xa + y * s2n, yb + x * s2n

    def remote(src, dst, k, i, peer):
        return pltpu.make_async_remote_copy(
            src_ref=src, dst_ref=dst, send_sem=ssem.at[k, i], recv_sem=rsem.at[k, i],
            device_id=peer, device_id_type=MESH,
        )

    def c_d(k):
        return [remote(
            pb.at[lax.rem(k, 2), :, pl.ds(al((1 - core) * half, half), half), :],
            q.at[lax.rem(k, SLOTS)], k, 0, to_core)]

    def q_at(k, start, size):
        return q.at[lax.rem(k, SLOTS), :, pl.ds(al(start, zn), size), :]

    def o_at(k, start, size):
        return o_hbm.at[k, :, pl.ds(al(core * half + start, zn), size), :]

    def c_s1(k):
        sl = lax.rem(k, SLOTS)
        return [
            remote(q_at(k, (1 - x) * s1n, s1n), r1.at[sl, 0], k, 1, to_x),
            remote(q_at(k, col + (1 - y) * s1n, s1n), r1.at[sl, 1], k, 2, to_y),
        ]

    def c_s2(k):
        sl = lax.rem(k, SLOTS)
        return [
            remote(q_at(k, xa + (1 - y) * s2n, s2n), r2.at[sl, 0], k, 3, to_y),
            remote(q_at(k, yb + (1 - x) * s2n, s2n), r2.at[sl, 1], k, 4, to_x),
        ]

    def c_z(k):
        sl = lax.rem(k, SLOTS)
        out = []
        for j in range(3):
            zz = lax.rem(z + j + 1, 4) * zn
            out.append(remote(q_at(k, xya + zz, zn), rz.at[sl, j, 0], k, 5 + 2 * j, to_z[j]))
            out.append(remote(q_at(k, yxb + zz, zn), rz.at[sl, j, 1], k, 6 + 2 * j, to_z[j]))
        return out

    def c_zg(k):
        out = []
        for j in range(3):
            for n, base in enumerate((xya, yxb)):
                at = base + z * zn
                out.append(remote(q_at(k, at, zn), o_at(k, at, zn), k, 11 + 2 * j + n, to_z[j]))
        return out

    def c_local(k):
        return [
            pltpu.make_async_copy(q_at(k, base + z * zn, zn), o_at(k, base + z * zn, zn), lsem.at[k, n])
            for n, base in enumerate((xya, yxb))
        ]

    def c_s2g(k):
        return [
            remote(o_at(k, xya, s2n), o_at(k, xya, s2n), k, 17, to_y),
            remote(o_at(k, yxb, s2n), o_at(k, yxb, s2n), k, 18, to_x),
        ]

    def c_s1g(k):
        return [
            remote(o_at(k, xa, s1n), o_at(k, xa, s1n), k, 19, to_x),
            remote(o_at(k, yb, s1n), o_at(k, yb, s1n), k, 20, to_y),
        ]

    def c_dg(k):
        return [remote(o_at(k, 0, half), o_at(k, 0, half), k, 21, to_core)]

    def start(copies):
        for copy in copies:
            copy.start()

    def wait(copies):
        for copy in copies:
            copy.wait()

    def q_add(k, at, size, value):
        sl = lax.rem(k, SLOTS)
        ds = pl.ds(al(at, zn), size)
        q[sl, :, ds, :] = q[sl, :, ds, :] + value

    def stage(g, name, action):
        t = g - OFF[name] - NRB
        k = lax.div(t, NRB)

        @pl.when((t >= 0) & (lax.rem(t, NRB) == 0) & (k < UNITS))
        def _():
            action(k)

    def do_d(k):
        @pl.when(k >= SLOTS)
        def _():
            pl.semaphore_wait(csem.at[lax.rem(k, SLOTS)], len(peers))
        start(c_d(k))

    def do_s1(k):
        wait(c_d(k))
        sl = lax.rem(k, SLOTS)
        q[sl] = q[sl] + pb[lax.rem(k, 2), :, pl.ds(al(core * half, half), half), :]
        start(c_s1(k))

    def do_s2(k):
        wait(c_s1(k))
        sl = lax.rem(k, SLOTS)
        q_add(k, xa, s1n, r1[sl, 0])
        q_add(k, yb, s1n, r1[sl, 1])
        start(c_s2(k))

    def do_z(k):
        wait(c_s2(k))
        sl = lax.rem(k, SLOTS)
        q_add(k, xya, s2n, r2[sl, 0])
        q_add(k, yxb, s2n, r2[sl, 1])
        start(c_z(k))

    def do_zg(k):
        wait(c_z(k))
        sl = lax.rem(k, SLOTS)
        for n, base in enumerate((xya, yxb)):
            ds = pl.ds(al(base + z * zn, zn), zn)
            total = (q[sl, :, ds, :] + rz[sl, 0, n]) + (rz[sl, 1, n] + rz[sl, 2, n])
            q[sl, :, ds, :] = total * (1.0 / 32.0)
        start(c_zg(k))
        start(c_local(k))

    def do_s2g(k):
        wait(c_zg(k))
        wait(c_local(k))

        @pl.when(k < UNITS - SLOTS)
        def _():
            for peer in peers:
                pl.semaphore_signal(csem.at[lax.rem(k, SLOTS)], inc=1, device_id=peer, device_id_type=MESH)
        start(c_s2g(k))

    def do_s1g(k):
        wait(c_s2g(k))
        start(c_s1g(k))

    def do_dg(k):
        wait(c_s1g(k))
        start(c_dg(k))

    def do_end(k):
        wait(c_dg(k))

    def comm(g):
        stage(g, "d", do_d)
        stage(g, "end", do_end)
        stage(g, "dg", do_dg)
        stage(g, "s1g", do_s1g)
        stage(g, "s2g", do_s2g)
        stage(g, "zg", do_zg)
        stage(g, "z", do_z)
        stage(g, "s2", do_s2)
        stage(g, "s1", do_s1)

    sub = rows // SUBS
    er = min(EROWS, sub)

    def first_step(g, carry):
        c, r = lax.div(g, NRB), lax.rem(g, NRB)
        par = lax.rem(c, 2)
        comm(g)

        @pl.when(g == 0)
        def _():
            w_copies[0].wait()
            w_copies[1].wait()

        @pl.when(c == 0)
        def _():
            h_copy(r).wait()
            g_copy(r).wait()

        @pl.when(r == 0)
        def _():
            pb[par] = jnp.zeros_like(pb[par])

        hf = ffc // 2

        def rows_of(j):
            return pl.ds(al(r * rows + j * sub, sub), sub), slice(j * sub, (j + 1) * sub)

        def front(j):
            ds, at = rows_of(j)

            def act(n):
                col = pl.ds(al(c * ffc + n * hf, hf), hf)
                ab[at, n * hf : (n + 1) * hf] = nn(h2[ds, :], w3[:, col]).astype(BF16)

            def up(n):
                col = pl.ds(al(c * ffc + n * hf, hf), hf)
                ub[at, n * hf : (n + 1) * hf] = nt(gx[ds, :], w4[col, :])

            return [functools.partial(f, n) for n in range(2) for f in (act, up)]

        def middle(j):
            def piece(i):
                at = slice(j * sub + i, j * sub + i + er)
                h3, da = gelu_both(ab[at, :].astype(F32))
                hb[at, :] = h3.astype(BF16)
                db[at, :] = (ub[at, :] * da).astype(BF16)

            return [functools.partial(piece, i) for i in range(0, sub, er)]

        def back(j):
            ds, at = rows_of(j)

            def p4():
                pb[par, 0] += tn(hb[at, :], gx[ds, :])

            def p3():
                pb[par, 1] += tn(h2[ds, :], db[at, :])

            def down():
                prev = jnp.where(c == 0, gx[ds, :].astype(F32), dh[ds, :])
                dh[ds, :] = prev + nt(db[at, :], w3[:, pl.ds(al(c * ffc, ffc), ffc)])

            return [p4, p3, down]

        pipelined(SUBS, front, middle, back)

        @pl.when(c == NCH - 1)
        def _():
            h2[block(r), :] = dh[block(r), :].astype(BF16)
            x_copy(r).start()
        return carry

    def second_step(g, carry):
        i0 = g - NCH * NRB
        c, r = lax.div(i0, NRB), lax.rem(i0, NRB)
        par = lax.rem(c, 2)
        slot = lax.rem(i0, 2)

        @pl.when(i0 + 1 < NCH * NRB)
        def _():
            a_copy(i0 + 1).start()
        comm(g)

        @pl.when(c == 0)
        def _():
            x_copy(r).wait()

        @pl.when(r == 0)
        def _():
            pb[par] = jnp.zeros_like(pb[par])
        a_copy(i0).wait()

        def rows_of(j):
            return pl.ds(al(r * rows + j * sub, sub), sub), slice(j * sub, (j + 1) * sub)

        def front(j):
            ds, at = rows_of(j)

            def up():
                ub[at, :] = nt(h2[ds, :], w2[pl.ds(al(c * ffc, ffc), ffc), :])

            return [up]

        def middle(j):
            def piece(i):
                at = slice(j * sub + i, j * sub + i + er)
                h1, da = gelu_both(a1b[slot, at, :].astype(F32))
                hb[at, :] = h1.astype(BF16)
                db[at, :] = (ub[at, :] * da).astype(BF16)

            return [functools.partial(piece, i) for i in range(0, sub, er)]

        def back(j):
            ds, at = rows_of(j)

            def p2():
                pb[par, 0] += tn(hb[at, :], h2[ds, :])

            def p1():
                pb[par, 1] += tn(gx[ds, :], db[at, :])

            return [p2, p1]

        pipelined(SUBS, front, middle, back)
        return carry

    steps = NCH * NRB
    lax.fori_loop(0, steps, first_step, 0)
    w_copies[2].wait()
    lax.fori_loop(steps, 2 * steps, second_step, 0)

    def drain(g, carry):
        comm(g)
        return carry

    lax.fori_loop(2 * steps, 2 * steps + OFF["end"] + 1, drain, 0)


def finish_kernel(o_hbm, d1, d2, d3, d4, buf, isem, osem):
    half = UNITS // 2
    d, ffc = buf.shape[2], buf.shape[3]
    loads = [pltpu.make_async_copy(o_hbm.at[k], buf.at[k], isem.at[k]) for k in range(UNITS)]
    for copy in loads:
        copy.start()
    stores = []
    for k in range(UNITS):
        loads[k].wait()
        tall, wide = (d4, d3) if k < half else (d2, d1)
        at = pl.ds((k % half) * ffc, ffc)
        stores.append(pltpu.make_async_copy(buf.at[k, 0], tall.at[at, :], osem.at[k, 0]))
        stores.append(pltpu.make_async_copy(buf.at[k, 1], wide.at[:, at], osem.at[k, 1]))
        stores[-2].start()
        stores[-1].start()
    for copy in stores:
        copy.wait()


def solution(mesh):
    batch_spec = P(("z", "y", "xc"), None)
    whole_spec = P(None, None)
    any_spec = pl.BlockSpec(memory_space=pl.ANY)

    def device_step(x_loc, g_loc, w_one, w_two, w_three, w_four):
        n, d = x_loc.shape
        ff = w_one.shape[1]
        rows, ffc = n // NRB, ff // NCH
        mm = 2 * n * d * ff
        a1, h2 = pl.pallas_call(
            fwd_kernel,
            grid=(NRB,),
            in_specs=[
                pl.BlockSpec((rows, d), lambda i: (i, 0)),
                pl.BlockSpec((d, ff), lambda i: (0, 0)),
                pl.BlockSpec((ff, d), lambda i: (0, 0)),
            ],
            out_specs=[
                pl.BlockSpec((rows, ff), lambda i: (i, 0)),
                pl.BlockSpec((rows, d), lambda i: (i, 0)),
            ],
            out_shape=[jax.ShapeDtypeStruct((n, ff), BF16), jax.ShapeDtypeStruct((n, d), BF16)],
            scratch_shapes=[pltpu.VMEM((rows, ff), BF16), pltpu.VMEM((rows, d), F32)],
            compiler_params=pltpu.CompilerParams(vmem_limit_bytes=VMEM_LIMIT),
            cost_estimate=pl.CostEstimate(flops=2 * mm, bytes_accessed=2 * n * (ff + 2 * d), transcendentals=n * ff),
            name="fwd",
        )(x_loc, w_one, w_two)

        out = pl.pallas_call(
            grad_kernel,
            in_specs=[any_spec] * 7,
            out_specs=any_spec,
            out_shape=jax.ShapeDtypeStruct((UNITS, 2, d, ffc), F32),
            scratch_shapes=[
                pltpu.VMEM((n, d), BF16),
                pltpu.VMEM((n, d), BF16),
                pltpu.VMEM((n, d), F32),
                pltpu.VMEM((ff, d), BF16),
                pltpu.VMEM((d, ff), BF16),
                pltpu.VMEM((ff, d), BF16),
                pltpu.VMEM((2, rows, ffc), BF16),
                pltpu.VMEM((rows, ffc), BF16),
                pltpu.VMEM((rows, ffc), F32),
                pltpu.VMEM((rows, ffc), BF16),
                pltpu.VMEM((rows, ffc), BF16),
                pltpu.VMEM((2, 2, d, ffc), F32),
                pltpu.VMEM((SLOTS, 2, d // 2, ffc), F32),
                pltpu.VMEM((SLOTS, 2, 2, d // 8, ffc), F32),
                pltpu.VMEM((SLOTS, 2, 2, d // 16, ffc), F32),
                pltpu.VMEM((SLOTS, 3, 2, 2, d // 64, ffc), F32),
                pltpu.SemaphoreType.DMA((3,)),
                pltpu.SemaphoreType.DMA((NRB,)),
                pltpu.SemaphoreType.DMA((NRB,)),
                pltpu.SemaphoreType.DMA((NRB,)),
                pltpu.SemaphoreType.DMA((2,)),
                pltpu.SemaphoreType.DMA((UNITS, 2)),
                pltpu.SemaphoreType.DMA((UNITS, 22)),
                pltpu.SemaphoreType.DMA((UNITS, 22)),
                pltpu.SemaphoreType.REGULAR((SLOTS,)),
            ],
            compiler_params=pltpu.CompilerParams(
                collective_id=0, has_side_effects=True, vmem_limit_bytes=VMEM_LIMIT
            ),
            cost_estimate=pl.CostEstimate(flops=8 * mm, bytes_accessed=2 * n * (ff + 3 * d), transcendentals=2 * n * ff),
            name="grads",
        )(x_loc, g_loc, h2, a1, w_two, w_three, w_four)

        wide, tall = jax.ShapeDtypeStruct((d, ff), F32), jax.ShapeDtypeStruct((ff, d), F32)
        return pl.pallas_call(
            finish_kernel,
            in_specs=[any_spec],
            out_specs=[any_spec] * 4,
            out_shape=[wide, tall, wide, tall],
            scratch_shapes=[
                pltpu.VMEM((UNITS, 2, d, ffc), F32),
                pltpu.SemaphoreType.DMA((UNITS,)),
                pltpu.SemaphoreType.DMA((UNITS, 2)),
            ],
            compiler_params=pltpu.CompilerParams(vmem_limit_bytes=VMEM_LIMIT),
            name="finish",
        )(out)

    return jax.shard_map(
        device_step,
        mesh=mesh,
        in_specs=(batch_spec, batch_spec, whole_spec, whole_spec, whole_spec, whole_spec),
        out_specs=(whole_spec, whole_spec, whole_spec, whole_spec),
        check_vma=False,
    )
```

```python
import functools
import math
import jax
import jax.numpy as jnp
from jax import lax
from jax.experimental import pallas as pl
from jax.experimental.pallas import tpu as pltpu
from jax.sharding import PartitionSpec as P

C0 = math.sqrt(2.0 / math.pi)
K0 = 0.044715
F32 = jnp.float32
BF16 = jnp.bfloat16
MESH = pl.DeviceIdType.MESH
VMEM_LIMIT = 67_000_000

NCF = 4
NRF = 8
NCH = 8
NRB = 4
UNITS = 2 * NCH
SLOTS = 8
SUBS = 4
EROWS = 16

OFF = dict(d=0, s1=2, s2=5, z=8, zg=12, s2g=16, s1g=19, dg=22, end=25)


def nn(a, b):
    return jnp.dot(a, b, preferred_element_type=F32)


def nt(a, b):
    return lax.dot_general(a, b, (((1,), (1,)), ((), ())), preferred_element_type=F32)


def tn(a, b):
    return lax.dot_general(a, b, (((0,), (0,)), ((), ())), preferred_element_type=F32)


def gelu_only(a):
    kq = (K0 * a) * a
    t = jnp.tanh((C0 * a) * (1.0 + kq))
    return a * (0.5 * t + 0.5)


def gelu_both(a):
    kq = (K0 * a) * a
    t = jnp.tanh((C0 * a) * (1.0 + kq))
    s = 0.5 * t + 0.5
    h = a * s
    grad = s + (h * (C0 - C0 * t)) * (1.0 + 3.0 * kq)
    return h, grad


def woven(first, second):
    order = [((i + 0.5) / len(first), 0, f) for i, f in enumerate(first)]
    order += [((i + 0.5) / len(second), 1, f) for i, f in enumerate(second)]
    for _, _, f in sorted(order, key=lambda e: e[:2]):
        f()


def pipelined(count, front, middle, back, back_first=True):
    for f in front(0):
        f()
    for j in range(count):
        around = [front(j + 1) if j + 1 < count else [], back(j - 1) if j else []]
        around = around[1] + around[0] if back_first else around[0] + around[1]
        woven(around, middle(j))
    for f in back(count - 1):
        f()


def fwd_kernel(x_ref, w1_ref, w2_ref, a1_ref, h2_ref, hb, acc):
    rows, d = x_ref.shape
    ffc = w1_ref.shape[1] // NCF
    half = rows // 2
    er = min(EROWS, half)

    def place(j):
        c, n = j // 2, j % 2
        return slice(c * ffc, (c + 1) * ffc), slice(n * half, (n + 1) * half), c

    def front(j):
        cols, at, c = place(j)

        def up():
            a1_ref[at, cols] = nn(x_ref[at, :], w1_ref[:, cols]).astype(BF16)

        return [up]

    def middle(j):
        cols, at, c = place(j)

        def piece(i):
            ds = slice(at.start + i, at.start + i + er)
            hb[ds, cols] = gelu_only(a1_ref[ds, cols].astype(F32)).astype(BF16)

        return [functools.partial(piece, i) for i in range(0, half, er)]

    def back(j):
        cols, at, c = place(j)

        def down():
            prev = x_ref[at, :].astype(F32) if c == 0 else acc[at, :]
            total = prev + nn(hb[at, cols], w2_ref[cols, :])
            if c == NCF - 1:
                h2_ref[at, :] = total.astype(BF16)
            else:
                acc[at, :] = total

        return [down]

    pipelined(2 * NCF, front, middle, back, back_first=False)


def grad_kernel(
    x_hbm, g_hbm, h2_hbm, a1_hbm, w2_hbm, w3_hbm, w4_hbm, o_hbm,
    h2, gx, dh, w2, w3, w4, a1b, ab, ub, hb, db, pb, q, r1, r2, rz,
    wsem, hsem, gsem, xsem, asem, lsem, ssem, rsem, csem,
):
    d = h2.shape[1]
    rows = h2.shape[0] // NRB
    ffc = w3.shape[1] // NCH
    half, col, s1n, s2n = ffc // 2, ffc // 4, ffc // 8, ffc // 16
    hd = d // 2

    xc, y, z = lax.axis_index("xc"), lax.axis_index("y"), lax.axis_index("z")
    x, core = lax.div(xc, 2), lax.rem(xc, 2)
    to_core = {"xc": xc + 1 - 2 * core}
    to_x = {"xc": core + 2 * (1 - x)}
    to_y = {"y": 1 - y}
    to_z = [{"z": lax.rem(z + j, 4)} for j in (1, 2, 3)]
    peers = [to_core, to_x, to_y] + to_z

    def al(v, m):
        return pl.multiple_of(v, m)

    def block(i):
        return pl.ds(al(i * rows, rows), rows)

    w_copies = [
        pltpu.make_async_copy(src, dst, wsem.at[i])
        for i, (src, dst) in enumerate(((w3_hbm, w3), (w4_hbm, w4), (w2_hbm, w2)))
    ]

    def h_copy(i):
        return pltpu.make_async_copy(h2_hbm.at[block(i)], h2.at[block(i)], hsem.at[i])

    def g_copy(i):
        return pltpu.make_async_copy(g_hbm.at[block(i)], gx.at[block(i)], gsem.at[i])

    def x_copy(i):
        return pltpu.make_async_copy(x_hbm.at[block(i)], gx.at[block(i)], xsem.at[i])

    def a_copy(i):
        c, r = lax.div(i, NRB), lax.rem(i, NRB)
        slot = lax.rem(i, 2)
        return pltpu.make_async_copy(
            a1_hbm.at[block(r), pl.ds(al(c * ffc, ffc), ffc)], a1b.at[slot], asem.at[slot]
        )

    w_copies[0].start()
    h_copy(0).start()
    w_copies[1].start()
    g_copy(0).start()
    for i in range(1, NRB):
        h_copy(i).start()
        g_copy(i).start()
    w_copies[2].start()
    a_copy(jnp.int32(0)).start()

    barrier = pltpu.get_barrier_semaphore()
    for peer in peers:
        pl.semaphore_signal(barrier, inc=1, device_id=peer, device_id_type=MESH)
    pl.semaphore_wait(barrier, len(peers))

    xa, yb = x * s1n, col + y * s1n
    xya, yxb = xa + y * s2n, yb + x * s2n

    def remote(src, dst, k, i, peer):
        return pltpu.make_async_remote_copy(
            src_ref=src, dst_ref=dst, send_sem=ssem.at[lax.rem(k, SLOTS), i], recv_sem=rsem.at[lax.rem(k, SLOTS), i],
            device_id=peer, device_id_type=MESH,
        )

    def c_d(k):
        return [remote(
            pb.at[lax.rem(k, 2), :, pl.ds(al((1 - core) * half, half), half), :],
            q.at[lax.rem(k, SLOTS)], k, 0, to_core)]

    def q_at(k, start, size):
        return q.at[lax.rem(k, SLOTS), :, pl.ds(al(start, s2n), size), :]

    def o_at(k, start, size):
        return o_hbm.at[k, :, pl.ds(al(core * half + start, s2n), size), :]

    def c_s1(k):
        sl = lax.rem(k, SLOTS)
        return [
            remote(q_at(k, (1 - x) * s1n, s1n), r1.at[sl, 0], k, 1, to_x),
            remote(q_at(k, col + (1 - y) * s1n, s1n), r1.at[sl, 1], k, 2, to_y),
        ]

    def c_s2(k):
        sl = lax.rem(k, SLOTS)
        return [
            remote(q_at(k, xa + (1 - y) * s2n, s2n), r2.at[sl, 0], k, 3, to_y),
            remote(q_at(k, yb + (1 - x) * s2n, s2n), r2.at[sl, 1], k, 4, to_x),
        ]

    def z_piece(k, block, base):
        return q.at[lax.rem(k, SLOTS), block, pl.ds(al(base, s2n), s2n), :]

    def o_piece(k, base):
        return o_hbm.at[k, z, pl.ds(al(core * half + base, s2n), s2n), :]

    def c_z(k):
        sl = lax.rem(k, SLOTS)
        out = []
        for j in range(3):
            zz = lax.rem(z + j + 1, 4)
            for n, base in enumerate((xya, yxb)):
                out.append(remote(z_piece(k, zz, base), rz.at[sl, j, n], k, 5 + 2 * j + n, to_z[j]))
        return out

    def c_zg(k):
        out = []
        for j in range(3):
            for n, base in enumerate((xya, yxb)):
                out.append(remote(z_piece(k, z, base), o_piece(k, base), k, 11 + 2 * j + n, to_z[j]))
        return out

    def c_local(k):
        return [
            pltpu.make_async_copy(z_piece(k, z, base), o_piece(k, base), lsem.at[lax.rem(k, SLOTS), n])
            for n, base in enumerate((xya, yxb))
        ]

    def c_s2g(k):
        return [
            remote(o_at(k, xya, s2n), o_at(k, xya, s2n), k, 17, to_y),
            remote(o_at(k, yxb, s2n), o_at(k, yxb, s2n), k, 18, to_x),
        ]

    def c_s1g(k):
        return [
            remote(o_at(k, xa, s1n), o_at(k, xa, s1n), k, 19, to_x),
            remote(o_at(k, yb, s1n), o_at(k, yb, s1n), k, 20, to_y),
        ]

    def c_dg(k):
        return [remote(o_at(k, 0, half), o_at(k, 0, half), k, 21, to_core)]

    def start(copies):
        for copy in copies:
            copy.start()

    def wait(copies):
        for copy in copies:
            copy.wait()

    def q_add(k, at, size, value):
        sl = lax.rem(k, SLOTS)
        ds = pl.ds(al(at, s2n), size)
        q[sl, :, ds, :] = q[sl, :, ds, :] + value

    def stage(g, name, action):
        t = g - OFF[name] - NRB
        k = lax.div(t, NRB)

        @pl.when((t >= 0) & (lax.rem(t, NRB) == 0) & (k < UNITS))
        def _():
            action(k)

    def do_d(k):
        @pl.when(k >= SLOTS)
        def _():
            pl.semaphore_wait(csem.at[lax.rem(k, SLOTS)], len(peers))
        start(c_d(k))

    def do_s1(k):
        wait(c_d(k))
        sl = lax.rem(k, SLOTS)
        q[sl] = q[sl] + pb[lax.rem(k, 2), :, pl.ds(al(core * half, half), half), :]
        start(c_s1(k))

    def do_s2(k):
        wait(c_s1(k))
        sl = lax.rem(k, SLOTS)
        q_add(k, xa, s1n, r1[sl, 0])
        q_add(k, yb, s1n, r1[sl, 1])
        start(c_s2(k))

    def do_z(k):
        wait(c_s2(k))
        sl = lax.rem(k, SLOTS)
        q_add(k, xya, s2n, r2[sl, 0])
        q_add(k, yxb, s2n, r2[sl, 1])
        start(c_z(k))

    def do_zg(k):
        wait(c_z(k))
        sl = lax.rem(k, SLOTS)
        for n, base in enumerate((xya, yxb)):
            ds = pl.ds(al(base, s2n), s2n)
            total = (q[sl, z, ds, :] + rz[sl, 0, n]) + (rz[sl, 1, n] + rz[sl, 2, n])
            q[sl, z, ds, :] = total * (1.0 / 32.0)
        start(c_zg(k))
        start(c_local(k))

    def do_s2g(k):
        wait(c_zg(k))
        wait(c_local(k))

        @pl.when(k < UNITS - SLOTS)
        def _():
            for peer in peers:
                pl.semaphore_signal(csem.at[lax.rem(k, SLOTS)], inc=1, device_id=peer, device_id_type=MESH)
        start(c_s2g(k))

    def do_s1g(k):
        wait(c_s2g(k))
        start(c_s1g(k))

    def do_dg(k):
        wait(c_s1g(k))
        start(c_dg(k))

    def do_end(k):
        wait(c_dg(k))

    def comm(g):
        stage(g, "d", do_d)
        stage(g, "end", do_end)
        stage(g, "dg", do_dg)
        stage(g, "s1g", do_s1g)
        stage(g, "s2g", do_s2g)
        stage(g, "zg", do_zg)
        stage(g, "z", do_z)
        stage(g, "s2", do_s2)
        stage(g, "s1", do_s1)

    sub = rows // SUBS
    er = min(EROWS, sub)
    sub2 = sub // 2

    def first_step(g, carry):
        c, r = lax.div(g, NRB), lax.rem(g, NRB)
        par = lax.rem(c, 2)
        comm(g)

        @pl.when(g == 0)
        def _():
            w_copies[0].wait()
            w_copies[1].wait()

        @pl.when(c == 0)
        def _():
            h_copy(r).wait()
            g_copy(r).wait()

        @pl.when(r == 0)
        def _():
            pb[par] = jnp.zeros_like(pb[par])

        cols = pl.ds(al(c * ffc, ffc), ffc)
        hs = sub // 2

        def rows_of(j):
            return pl.ds(al(r * rows + j * sub, sub), sub), slice(j * sub, (j + 1) * sub)

        def front(j):
            def act(n):
                ds, at = pl.ds(al(r * rows + j * sub + n * hs, hs), hs), slice(j * sub + n * hs, j * sub + (n + 1) * hs)
                ab[at, :] = nn(h2[ds, :], w3[:, cols]).astype(BF16)

            def up(n):
                ds, at = pl.ds(al(r * rows + j * sub + n * hs, hs), hs), slice(j * sub + n * hs, j * sub + (n + 1) * hs)
                ub[at, :] = nt(gx[ds, :], w4[cols, :])

            return [functools.partial(f, n) for n in range(2) for f in (act, up)]

        def middle(j):
            def piece(i):
                at = slice(j * sub + i, j * sub + i + er)
                h3, da = gelu_both(ab[at, :].astype(F32))
                hb[at, :] = h3.astype(BF16)
                db[at, :] = (ub[at, :] * da).astype(BF16)

            return [functools.partial(piece, i) for i in range(0, sub, er)]

        def back(j):
            ds, at = rows_of(j)

            def p4():
                part = tn(hb[at, :], gx[ds, :])
                pb[par, 0] += part[:, :hd]
                pb[par, 1] += part[:, hd:]

            def p3():
                part = tn(h2[ds, :], db[at, :])
                pb[par, 2] += part[:hd]
                pb[par, 3] += part[hd:]

            def down():
                prev = jnp.where(c == 0, gx[ds, :].astype(F32), dh[ds, :])
                dh[ds, :] = prev + nt(db[at, :], w3[:, cols])

            return [p4, p3, down]

        pipelined(SUBS, front, middle, back)

        @pl.when(c == NCH - 1)
        def _():
            h2[block(r), :] = dh[block(r), :].astype(BF16)
            x_copy(r).start()
        return carry

    def second_step(g, carry):
        i0 = g - NCH * NRB
        c, r = lax.div(i0, NRB), lax.rem(i0, NRB)
        par = lax.rem(c, 2)
        slot = lax.rem(i0, 2)

        @pl.when(i0 + 1 < NCH * NRB)
        def _():
            a_copy(i0 + 1).start()
        comm(g)

        @pl.when(c == 0)
        def _():
            x_copy(r).wait()

        @pl.when(r == 0)
        def _():
            pb[par] = jnp.zeros_like(pb[par])
        a_copy(i0).wait()

        def rows_of(j):
            return pl.ds(al(r * rows + j * sub2, sub2), sub2), slice(j * sub2, (j + 1) * sub2)

        def front(j):
            ds, at = rows_of(j)

            def up():
                ub[at, :] = nt(h2[ds, :], w2[pl.ds(al(c * ffc, ffc), ffc), :])

            return [up]

        def middle(j):
            def piece(i):
                at = slice(j * sub2 + i, j * sub2 + i + er)
                h1, da = gelu_both(a1b[slot, at, :].astype(F32))
                hb[at, :] = h1.astype(BF16)
                db[at, :] = (ub[at, :] * da).astype(BF16)

            return [functools.partial(piece, i) for i in range(0, sub2, er)]

        def back(j):
            ds, at = rows_of(j)

            def p2():
                part = tn(hb[at, :], h2[ds, :])
                pb[par, 0] += part[:, :hd]
                pb[par, 1] += part[:, hd:]

            def p1():
                part = tn(gx[ds, :], db[at, :])
                pb[par, 2] += part[:hd]
                pb[par, 3] += part[hd:]

            return [p2, p1]

        pipelined(2 * SUBS, front, middle, back, back_first=False)
        return carry

    steps = NCH * NRB
    lax.fori_loop(0, steps, first_step, 0)
    w_copies[2].wait()
    lax.fori_loop(steps, 2 * steps, second_step, 0)

    def drain(g, carry):
        comm(g)
        return carry

    lax.fori_loop(2 * steps, 2 * steps + OFF["end"] + 1, drain, 0)


def finish_kernel(o_hbm, d1, d2, d3, d4, buf, isem, osem):
    half = UNITS // 2
    ffc, hd = buf.shape[2], buf.shape[3]
    loads = [pltpu.make_async_copy(o_hbm.at[k], buf.at[k], isem.at[k]) for k in range(UNITS)]
    for copy in loads:
        copy.start()
    stores = []
    for k in range(UNITS):
        loads[k].wait()
        tall, wide = (d4, d3) if k < half else (d2, d1)
        at = pl.ds((k % half) * ffc, ffc)
        for n in range(2):
            side = pl.ds(n * hd, hd)
            stores.append(pltpu.make_async_copy(buf.at[k, n], tall.at[at, side], osem.at[k, n]))
            stores.append(pltpu.make_async_copy(buf.at[k, 2 + n], wide.at[side, at], osem.at[k, 2 + n]))
            stores[-2].start()
            stores[-1].start()
    for copy in stores:
        copy.wait()


def solution(mesh):
    batch_spec = P(("z", "y", "xc"), None)
    whole_spec = P(None, None)
    any_spec = pl.BlockSpec(memory_space=pl.ANY)

    def device_step(x_loc, g_loc, w_one, w_two, w_three, w_four):
        n, d = x_loc.shape
        ff = w_one.shape[1]
        rows, ffc, frows = n // NRB, ff // NCH, n // NRF
        mm = 2 * n * d * ff
        a1, h2 = pl.pallas_call(
            fwd_kernel,
            grid=(NRF,),
            in_specs=[
                pl.BlockSpec((frows, d), lambda i: (i, 0)),
                pl.BlockSpec((d, ff), lambda i: (0, 0)),
                pl.BlockSpec((ff, d), lambda i: (0, 0)),
            ],
            out_specs=[
                pl.BlockSpec((frows, ff), lambda i: (i, 0)),
                pl.BlockSpec((frows, d), lambda i: (i, 0)),
            ],
            out_shape=[jax.ShapeDtypeStruct((n, ff), BF16), jax.ShapeDtypeStruct((n, d), BF16)],
            scratch_shapes=[pltpu.VMEM((frows, ff), BF16), pltpu.VMEM((frows, d), F32)],
            compiler_params=pltpu.CompilerParams(vmem_limit_bytes=VMEM_LIMIT),
            cost_estimate=pl.CostEstimate(flops=2 * mm, bytes_accessed=2 * n * (ff + 2 * d), transcendentals=n * ff),
            name="fwd",
        )(x_loc, w_one, w_two)

        out = pl.pallas_call(
            grad_kernel,
            in_specs=[any_spec] * 7,
            out_specs=any_spec,
            out_shape=jax.ShapeDtypeStruct((UNITS, 4, ffc, d // 2), F32),
            scratch_shapes=[
                pltpu.VMEM((n, d), BF16),
                pltpu.VMEM((n, d), BF16),
                pltpu.VMEM((n, d), F32),
                pltpu.VMEM((ff, d), BF16),
                pltpu.VMEM((d, ff), BF16),
                pltpu.VMEM((ff, d), BF16),
                pltpu.VMEM((2, rows, ffc), BF16),
                pltpu.VMEM((rows, ffc), BF16),
                pltpu.VMEM((rows, ffc), F32),
                pltpu.VMEM((rows, ffc), BF16),
                pltpu.VMEM((rows, ffc), BF16),
                pltpu.VMEM((2, 4, ffc, d // 2), F32),
                pltpu.VMEM((SLOTS, 4, ffc // 2, d // 2), F32),
                pltpu.VMEM((SLOTS, 2, 4, ffc // 8, d // 2), F32),
                pltpu.VMEM((SLOTS, 2, 4, ffc // 16, d // 2), F32),
                pltpu.VMEM((SLOTS, 3, 2, ffc // 16, d // 2), F32),
                pltpu.SemaphoreType.DMA((3,)),
                pltpu.SemaphoreType.DMA((NRB,)),
                pltpu.SemaphoreType.DMA((NRB,)),
                pltpu.SemaphoreType.DMA((NRB,)),
                pltpu.SemaphoreType.DMA((2,)),
                pltpu.SemaphoreType.DMA((SLOTS, 2)),
                pltpu.SemaphoreType.DMA((SLOTS, 22)),
                pltpu.SemaphoreType.DMA((SLOTS, 22)),
                pltpu.SemaphoreType.REGULAR((SLOTS,)),
            ],
            compiler_params=pltpu.CompilerParams(
                collective_id=0, has_side_effects=True, vmem_limit_bytes=VMEM_LIMIT
            ),
            cost_estimate=pl.CostEstimate(flops=8 * mm, bytes_accessed=2 * n * (ff + 3 * d), transcendentals=2 * n * ff),
            name="grads",
        )(x_loc, g_loc, h2, a1, w_two, w_three, w_four)

        wide, tall = jax.ShapeDtypeStruct((d, ff), F32), jax.ShapeDtypeStruct((ff, d), F32)
        return pl.pallas_call(
            finish_kernel,
            in_specs=[any_spec],
            out_specs=[any_spec] * 4,
            out_shape=[wide, tall, wide, tall],
            scratch_shapes=[
                pltpu.VMEM((UNITS, 4, ffc, d // 2), F32),
                pltpu.SemaphoreType.DMA((UNITS,)),
                pltpu.SemaphoreType.DMA((UNITS, 4)),
            ],
            compiler_params=pltpu.CompilerParams(vmem_limit_bytes=VMEM_LIMIT),
            name="finish",
        )(out)

    return jax.shard_map(
        device_step,
        mesh=mesh,
        in_specs=(batch_spec, batch_spec, whole_spec, whole_spec, whole_spec, whole_spec),
        out_specs=(whole_spec, whole_spec, whole_spec, whole_spec),
        check_vma=False,
    )
```

```python
import functools
import math
import jax
import jax.numpy as jnp
from jax import lax
from jax.experimental import pallas as pl
from jax.experimental.pallas import tpu as pltpu
from jax.sharding import PartitionSpec as P

C0 = math.sqrt(2.0 / math.pi)
K0 = 0.044715
F32 = jnp.float32
BF16 = jnp.bfloat16
MESH = pl.DeviceIdType.MESH
VMEM_LIMIT = 67_000_000

NCF = 4
NRF = 8
NCH = 8
NRB = 4
UNITS = 2 * NCH
SLOTS = 8
SUBS = 4
EROWS = 16

OFF = dict(
    d=(0, 0), s1=(1, 2), s2=(3, 5), z=(5, 8), zg=(8, 11), s2g=(11, 15), s1g=(13, 18), dg=(15, 21), end=(17, 24)
)
EARLY = 6
LAST = OFF["end"][1]


def nn(a, b):
    return jnp.dot(a, b, preferred_element_type=F32)


def nt(a, b):
    return lax.dot_general(a, b, (((1,), (1,)), ((), ())), preferred_element_type=F32)


def tn(a, b):
    return lax.dot_general(a, b, (((0,), (0,)), ((), ())), preferred_element_type=F32)


def gelu_only(a):
    kq = (K0 * a) * a
    t = jnp.tanh((C0 * a) * (1.0 + kq))
    return a * (0.5 * t + 0.5)


def gelu_both(a):
    kq = (K0 * a) * a
    t = jnp.tanh((C0 * a) * (1.0 + kq))
    s = 0.5 * t + 0.5
    h = a * s
    grad = s + (h * (C0 - C0 * t)) * (1.0 + 3.0 * kq)
    return h, grad


def woven(first, second):
    order = [((i + 0.5) / len(first), 0, f) for i, f in enumerate(first)]
    order += [((i + 0.5) / len(second), 1, f) for i, f in enumerate(second)]
    for _, _, f in sorted(order, key=lambda e: e[:2]):
        f()


def pipelined(count, front, middle, back, back_first=True):
    for f in front(0):
        f()
    for j in range(count):
        around = [front(j + 1) if j + 1 < count else [], back(j - 1) if j else []]
        around = around[1] + around[0] if back_first else around[0] + around[1]
        woven(around, middle(j))
    for f in back(count - 1):
        f()


def fwd_kernel(x_ref, w1_ref, w2_ref, a1_ref, h2_ref, hb, acc):
    rows, d = x_ref.shape
    ffc = w1_ref.shape[1] // NCF
    half = rows // 2
    er = min(EROWS, half)

    def place(j):
        c, n = j // 2, j % 2
        return slice(c * ffc, (c + 1) * ffc), slice(n * half, (n + 1) * half), c

    def front(j):
        cols, at, c = place(j)

        def up():
            a1_ref[at, cols] = nn(x_ref[at, :], w1_ref[:, cols]).astype(BF16)

        return [up]

    def middle(j):
        cols, at, c = place(j)

        def piece(i):
            ds = slice(at.start + i, at.start + i + er)
            hb[ds, cols] = gelu_only(a1_ref[ds, cols].astype(F32)).astype(BF16)

        return [functools.partial(piece, i) for i in range(0, half, er)]

    def back(j):
        cols, at, c = place(j)

        def down():
            prev = x_ref[at, :].astype(F32) if c == 0 else acc[at, :]
            total = prev + nn(hb[at, cols], w2_ref[cols, :])
            if c == NCF - 1:
                h2_ref[at, :] = total.astype(BF16)
            else:
                acc[at, :] = total

        return [down]

    pipelined(2 * NCF, front, middle, back, back_first=False)


def grad_kernel(
    x_hbm, g_hbm, h2_hbm, a1_hbm, w2_hbm, w3_hbm, w4_hbm, o_hbm,
    h2, gx, dh, w2, w3, w4, a1b, ab, ub, hb, db, pb, q, r1, r2, rz,
    wsem, hsem, gsem, xsem, asem, lsem, ssem, rsem, csem,
):
    d = h2.shape[1]
    rows = h2.shape[0] // NRB
    ffc = w3.shape[1] // NCH
    half, col, s1n, s2n = ffc // 2, ffc // 4, ffc // 8, ffc // 16
    hd = d // 2

    xc, y, z = lax.axis_index("xc"), lax.axis_index("y"), lax.axis_index("z")
    x, core = lax.div(xc, 2), lax.rem(xc, 2)
    to_core = {"xc": xc + 1 - 2 * core}
    to_x = {"xc": core + 2 * (1 - x)}
    to_y = {"y": 1 - y}
    to_z = [{"z": lax.rem(z + j, 4)} for j in (1, 2, 3)]
    peers = [to_core, to_x, to_y] + to_z

    def al(v, m):
        return pl.multiple_of(v, m)

    def block(i):
        return pl.ds(al(i * rows, rows), rows)

    w_copies = [
        pltpu.make_async_copy(src, dst, wsem.at[i])
        for i, (src, dst) in enumerate(((w3_hbm, w3), (w4_hbm, w4), (w2_hbm, w2)))
    ]

    def h_copy(i):
        return pltpu.make_async_copy(h2_hbm.at[block(i)], h2.at[block(i)], hsem.at[i])

    def g_copy(i):
        return pltpu.make_async_copy(g_hbm.at[block(i)], gx.at[block(i)], gsem.at[i])

    def x_copy(i):
        return pltpu.make_async_copy(x_hbm.at[block(i)], gx.at[block(i)], xsem.at[i])

    def a_copy(i):
        c, r = lax.div(i, NRB), lax.rem(i, NRB)
        slot = lax.rem(i, 2)
        return pltpu.make_async_copy(
            a1_hbm.at[block(r), pl.ds(al(c * ffc, ffc), ffc)], a1b.at[slot], asem.at[slot]
        )

    w_copies[0].start()
    h_copy(0).start()
    w_copies[1].start()
    g_copy(0).start()
    for i in range(1, NRB):
        h_copy(i).start()
        g_copy(i).start()
    w_copies[2].start()
    a_copy(jnp.int32(0)).start()

    barrier = pltpu.get_barrier_semaphore()
    for peer in peers:
        pl.semaphore_signal(barrier, inc=1, device_id=peer, device_id_type=MESH)
    pl.semaphore_wait(barrier, len(peers))

    xa, yb = x * s1n, col + y * s1n
    xya, yxb = xa + y * s2n, yb + x * s2n

    def remote(src, dst, k, i, peer):
        return pltpu.make_async_remote_copy(
            src_ref=src, dst_ref=dst, send_sem=ssem.at[lax.rem(k, SLOTS), i], recv_sem=rsem.at[lax.rem(k, SLOTS), i],
            device_id=peer, device_id_type=MESH,
        )

    def c_d(k):
        return [remote(
            pb.at[lax.rem(k, 2), :, pl.ds(al((1 - core) * half, half), half), :],
            q.at[lax.rem(k, SLOTS)], k, 0, to_core)]

    def q_at(k, start, size):
        return q.at[lax.rem(k, SLOTS), :, pl.ds(al(start, s2n), size), :]

    def o_at(k, start, size):
        return o_hbm.at[k, :, pl.ds(al(core * half + start, s2n), size), :]

    def c_s1(k):
        sl = lax.rem(k, SLOTS)
        return [
            remote(q_at(k, (1 - x) * s1n, s1n), r1.at[sl, 0], k, 1, to_x),
            remote(q_at(k, col + (1 - y) * s1n, s1n), r1.at[sl, 1], k, 2, to_y),
        ]

    def c_s2(k):
        sl = lax.rem(k, SLOTS)
        return [
            remote(q_at(k, xa + (1 - y) * s2n, s2n), r2.at[sl, 0], k, 3, to_y),
            remote(q_at(k, yb + (1 - x) * s2n, s2n), r2.at[sl, 1], k, 4, to_x),
        ]

    def z_piece(k, block, base):
        return q.at[lax.rem(k, SLOTS), block, pl.ds(al(base, s2n), s2n), :]

    def o_piece(k, base):
        return o_hbm.at[k, z, pl.ds(al(core * half + base, s2n), s2n), :]

    def c_z(k):
        sl = lax.rem(k, SLOTS)
        out = []
        for j in range(3):
            zz = lax.rem(z + j + 1, 4)
            for n, base in enumerate((xya, yxb)):
                out.append(remote(z_piece(k, zz, base), rz.at[sl, j, n], k, 5 + 2 * j + n, to_z[j]))
        return out

    def c_zg(k):
        out = []
        for j in range(3):
            for n, base in enumerate((xya, yxb)):
                out.append(remote(z_piece(k, z, base), o_piece(k, base), k, 11 + 2 * j + n, to_z[j]))
        return out

    def c_local(k):
        return [
            pltpu.make_async_copy(z_piece(k, z, base), o_piece(k, base), lsem.at[lax.rem(k, SLOTS), n])
            for n, base in enumerate((xya, yxb))
        ]

    def c_s2g(k):
        return [
            remote(o_at(k, xya, s2n), o_at(k, xya, s2n), k, 17, to_y),
            remote(o_at(k, yxb, s2n), o_at(k, yxb, s2n), k, 18, to_x),
        ]

    def c_s1g(k):
        return [
            remote(o_at(k, xa, s1n), o_at(k, xa, s1n), k, 19, to_x),
            remote(o_at(k, yb, s1n), o_at(k, yb, s1n), k, 20, to_y),
        ]

    def c_dg(k):
        return [remote(o_at(k, 0, half), o_at(k, 0, half), k, 21, to_core)]

    def start(copies):
        for copy in copies:
            copy.start()

    def wait(copies):
        for copy in copies:
            copy.wait()

    def q_add(k, at, size, value):
        sl = lax.rem(k, SLOTS)
        ds = pl.ds(al(at, s2n), size)
        q[sl, :, ds, :] = q[sl, :, ds, :] + value

    def stage(g, name, action):
        early, late = OFF[name]
        te, tl = g - early - NRB, g - late - NRB
        ke, kl = lax.div(te, NRB), lax.div(tl, NRB)
        is_e = (te >= 0) & (lax.rem(te, NRB) == 0) & (ke < EARLY)
        is_l = (tl >= 0) & (lax.rem(tl, NRB) == 0) & (kl >= EARLY) & (kl < UNITS)
        k = jnp.where(is_e, ke, kl)

        @pl.when(is_e | is_l)
        def _():
            action(k)

    def do_d(k):
        @pl.when(k >= SLOTS)
        def _():
            pl.semaphore_wait(csem.at[lax.rem(k, SLOTS)], len(peers))
        start(c_d(k))

    def do_s1(k):
        wait(c_d(k))
        sl = lax.rem(k, SLOTS)
        q[sl] = q[sl] + pb[lax.rem(k, 2), :, pl.ds(al(core * half, half), half), :]
        start(c_s1(k))

    def do_s2(k):
        wait(c_s1(k))
        sl = lax.rem(k, SLOTS)
        q_add(k, xa, s1n, r1[sl, 0])
        q_add(k, yb, s1n, r1[sl, 1])
        start(c_s2(k))

    def do_z(k):
        wait(c_s2(k))
        sl = lax.rem(k, SLOTS)
        q_add(k, xya, s2n, r2[sl, 0])
        q_add(k, yxb, s2n, r2[sl, 1])
        start(c_z(k))

    def do_zg(k):
        wait(c_z(k))
        sl = lax.rem(k, SLOTS)
        for n, base in enumerate((xya, yxb)):
            ds = pl.ds(al(base, s2n), s2n)
            total = (q[sl, z, ds, :] + rz[sl, 0, n]) + (rz[sl, 1, n] + rz[sl, 2, n])
            q[sl, z, ds, :] = total * (1.0 / 32.0)
        start(c_zg(k))
        start(c_local(k))

    def do_s2g(k):
        wait(c_zg(k))
        wait(c_local(k))

        @pl.when(k < UNITS - SLOTS)
        def _():
            for peer in peers:
                pl.semaphore_signal(csem.at[lax.rem(k, SLOTS)], inc=1, device_id=peer, device_id_type=MESH)
        start(c_s2g(k))

    def do_s1g(k):
        wait(c_s2g(k))
        start(c_s1g(k))

    def do_dg(k):
        wait(c_s1g(k))
        start(c_dg(k))

    def do_end(k):
        wait(c_dg(k))

    def comm(g):
        stage(g, "d", do_d)
        stage(g, "end", do_end)
        stage(g, "dg", do_dg)
        stage(g, "s1g", do_s1g)
        stage(g, "s2g", do_s2g)
        stage(g, "zg", do_zg)
        stage(g, "z", do_z)
        stage(g, "s2", do_s2)
        stage(g, "s1", do_s1)

    sub = rows // SUBS
    er = min(EROWS, sub)
    sub2 = sub // 2

    def first_step(g, carry):
        c, r = lax.div(g, NRB), lax.rem(g, NRB)
        par = lax.rem(c, 2)
        comm(g)

        @pl.when(g == 0)
        def _():
            w_copies[0].wait()
            w_copies[1].wait()

        @pl.when(c == 0)
        def _():
            h_copy(r).wait()
            g_copy(r).wait()

        @pl.when(r == 0)
        def _():
            pb[par] = jnp.zeros_like(pb[par])

        cols = pl.ds(al(c * ffc, ffc), ffc)
        hs = sub // 2

        def rows_of(j):
            return pl.ds(al(r * rows + j * sub, sub), sub), slice(j * sub, (j + 1) * sub)

        def front(j):
            def act(n):
                ds, at = pl.ds(al(r * rows + j * sub + n * hs, hs), hs), slice(j * sub + n * hs, j * sub + (n + 1) * hs)
                ab[at, :] = nn(h2[ds, :], w3[:, cols]).astype(BF16)

            def up(n):
                ds, at = pl.ds(al(r * rows + j * sub + n * hs, hs), hs), slice(j * sub + n * hs, j * sub + (n + 1) * hs)
                ub[at, :] = nt(gx[ds, :], w4[cols, :])

            return [functools.partial(f, n) for n in range(2) for f in (act, up)]

        def middle(j):
            def piece(i):
                at = slice(j * sub + i, j * sub + i + er)
                h3, da = gelu_both(ab[at, :].astype(F32))
                hb[at, :] = h3.astype(BF16)
                db[at, :] = (ub[at, :] * da).astype(BF16)

            return [functools.partial(piece, i) for i in range(0, sub, er)]

        def back(j):
            ds, at = rows_of(j)

            def p4():
                part = tn(hb[at, :], gx[ds, :])
                pb[par, 0] += part[:, :hd]
                pb[par, 1] += part[:, hd:]

            def p3():
                part = tn(h2[ds, :], db[at, :])
                pb[par, 2] += part[:hd]
                pb[par, 3] += part[hd:]

            def down():
                prev = jnp.where(c == 0, gx[ds, :].astype(F32), dh[ds, :])
                dh[ds, :] = prev + nt(db[at, :], w3[:, cols])

            return [p3, p4, down]

        pipelined(SUBS, front, middle, back)

        @pl.when(c == NCH - 1)
        def _():
            h2[block(r), :] = dh[block(r), :].astype(BF16)
            x_copy(r).start()
        return carry

    def second_step(g, carry):
        i0 = g - NCH * NRB
        c, r = lax.div(i0, NRB), lax.rem(i0, NRB)
        par = lax.rem(c, 2)
        slot = lax.rem(i0, 2)

        @pl.when(i0 + 1 < NCH * NRB)
        def _():
            a_copy(i0 + 1).start()
        comm(g)

        @pl.when(c == 0)
        def _():
            x_copy(r).wait()

        @pl.when(r == 0)
        def _():
            pb[par] = jnp.zeros_like(pb[par])
        a_copy(i0).wait()

        def rows_of(j):
            return pl.ds(al(r * rows + j * sub2, sub2), sub2), slice(j * sub2, (j + 1) * sub2)

        def front(j):
            ds, at = rows_of(j)

            def up():
                ub[at, :] = nt(h2[ds, :], w2[pl.ds(al(c * ffc, ffc), ffc), :])

            return [up]

        def middle(j):
            def piece(i):
                at = slice(j * sub2 + i, j * sub2 + i + er)
                h1, da = gelu_both(a1b[slot, at, :].astype(F32))
                hb[at, :] = h1.astype(BF16)
                db[at, :] = (ub[at, :] * da).astype(BF16)

            return [functools.partial(piece, i) for i in range(0, sub2, er)]

        def back(j):
            ds, at = rows_of(j)

            def p2():
                part = tn(hb[at, :], h2[ds, :])
                pb[par, 0] += part[:, :hd]
                pb[par, 1] += part[:, hd:]

            def p1():
                part = tn(gx[ds, :], db[at, :])
                pb[par, 2] += part[:hd]
                pb[par, 3] += part[hd:]

            return [p2, p1]

        pipelined(2 * SUBS, front, middle, back, back_first=False)
        return carry

    steps = NCH * NRB
    lax.fori_loop(0, steps, first_step, 0)
    w_copies[2].wait()
    lax.fori_loop(steps, 2 * steps, second_step, 0)

    def drain(g, carry):
        comm(g)
        return carry

    lax.fori_loop(2 * steps, 2 * steps + LAST + 1, drain, 0)


def finish_kernel(o_hbm, d1, d2, d3, d4, buf, isem, osem):
    half = UNITS // 2
    ffc, hd = buf.shape[2], buf.shape[3]
    loads = [pltpu.make_async_copy(o_hbm.at[k], buf.at[k], isem.at[k]) for k in range(UNITS)]
    for copy in loads:
        copy.start()
    stores = []
    for k in range(UNITS):
        loads[k].wait()
        tall, wide = (d4, d3) if k < half else (d2, d1)
        at = pl.ds((k % half) * ffc, ffc)
        for n in range(2):
            side = pl.ds(n * hd, hd)
            stores.append(pltpu.make_async_copy(buf.at[k, n], tall.at[at, side], osem.at[k, n]))
            stores.append(pltpu.make_async_copy(buf.at[k, 2 + n], wide.at[side, at], osem.at[k, 2 + n]))
            stores[-2].start()
            stores[-1].start()
    for copy in stores:
        copy.wait()


def solution(mesh):
    batch_spec = P(("z", "y", "xc"), None)
    whole_spec = P(None, None)
    any_spec = pl.BlockSpec(memory_space=pl.ANY)

    def device_step(x_loc, g_loc, w_one, w_two, w_three, w_four):
        n, d = x_loc.shape
        ff = w_one.shape[1]
        rows, ffc, frows = n // NRB, ff // NCH, n // NRF
        mm = 2 * n * d * ff
        a1, h2 = pl.pallas_call(
            fwd_kernel,
            grid=(NRF,),
            in_specs=[
                pl.BlockSpec((frows, d), lambda i: (i, 0)),
                pl.BlockSpec((d, ff), lambda i: (0, 0)),
                pl.BlockSpec((ff, d), lambda i: (0, 0)),
            ],
            out_specs=[
                pl.BlockSpec((frows, ff), lambda i: (i, 0)),
                pl.BlockSpec((frows, d), lambda i: (i, 0)),
            ],
            out_shape=[jax.ShapeDtypeStruct((n, ff), BF16), jax.ShapeDtypeStruct((n, d), BF16)],
            scratch_shapes=[pltpu.VMEM((frows, ff), BF16), pltpu.VMEM((frows, d), F32)],
            compiler_params=pltpu.CompilerParams(vmem_limit_bytes=VMEM_LIMIT),
            cost_estimate=pl.CostEstimate(flops=2 * mm, bytes_accessed=2 * n * (ff + 2 * d), transcendentals=n * ff),
            name="fwd",
        )(x_loc, w_one, w_two)

        out = pl.pallas_call(
            grad_kernel,
            in_specs=[any_spec] * 7,
            out_specs=any_spec,
            out_shape=jax.ShapeDtypeStruct((UNITS, 4, ffc, d // 2), F32),
            scratch_shapes=[
                pltpu.VMEM((n, d), BF16),
                pltpu.VMEM((n, d), BF16),
                pltpu.VMEM((n, d), F32),
                pltpu.VMEM((ff, d), BF16),
                pltpu.VMEM((d, ff), BF16),
                pltpu.VMEM((ff, d), BF16),
                pltpu.VMEM((2, rows, ffc), BF16),
                pltpu.VMEM((rows, ffc), BF16),
                pltpu.VMEM((rows, ffc), F32),
                pltpu.VMEM((rows, ffc), BF16),
                pltpu.VMEM((rows, ffc), BF16),
                pltpu.VMEM((2, 4, ffc, d // 2), F32),
                pltpu.VMEM((SLOTS, 4, ffc // 2, d // 2), F32),
                pltpu.VMEM((SLOTS, 2, 4, ffc // 8, d // 2), F32),
                pltpu.VMEM((SLOTS, 2, 4, ffc // 16, d // 2), F32),
                pltpu.VMEM((SLOTS, 3, 2, ffc // 16, d // 2), F32),
                pltpu.SemaphoreType.DMA((3,)),
                pltpu.SemaphoreType.DMA((NRB,)),
                pltpu.SemaphoreType.DMA((NRB,)),
                pltpu.SemaphoreType.DMA((NRB,)),
                pltpu.SemaphoreType.DMA((2,)),
                pltpu.SemaphoreType.DMA((SLOTS, 2)),
                pltpu.SemaphoreType.DMA((SLOTS, 22)),
                pltpu.SemaphoreType.DMA((SLOTS, 22)),
                pltpu.SemaphoreType.REGULAR((SLOTS,)),
            ],
            compiler_params=pltpu.CompilerParams(
                collective_id=0, has_side_effects=True, vmem_limit_bytes=VMEM_LIMIT
            ),
            cost_estimate=pl.CostEstimate(flops=8 * mm, bytes_accessed=2 * n * (ff + 3 * d), transcendentals=2 * n * ff),
            name="grads",
        )(x_loc, g_loc, h2, a1, w_two, w_three, w_four)

        wide, tall = jax.ShapeDtypeStruct((d, ff), F32), jax.ShapeDtypeStruct((ff, d), F32)
        return pl.pallas_call(
            finish_kernel,
            in_specs=[any_spec],
            out_specs=[any_spec] * 4,
            out_shape=[wide, tall, wide, tall],
            scratch_shapes=[
                pltpu.VMEM((UNITS, 4, ffc, d // 2), F32),
                pltpu.SemaphoreType.DMA((UNITS,)),
                pltpu.SemaphoreType.DMA((UNITS, 4)),
            ],
            compiler_params=pltpu.CompilerParams(vmem_limit_bytes=VMEM_LIMIT),
            name="finish",
        )(out)

    return jax.shard_map(
        device_step,
        mesh=mesh,
        in_specs=(batch_spec, batch_spec, whole_spec, whole_spec, whole_spec, whole_spec),
        out_specs=(whole_spec, whole_spec, whole_spec, whole_spec),
        check_vma=False,
    )
```
